128 devices in a mesh: row: 8 (over x, z_hi), col: 4 (over z_lo, core), depth: 4 (over y).
Axes of the slice: x: 4, y: 4, z: 4 (z_hi: 2, z_lo: 2; z = z_hi * 2 + z_lo), core: 2. Of those that a mesh axis runs over, the one named last changes fastest.
Arguments:
- acts: bfloat16 [8192, 5120], P(('depth', 'col'), 'row'), may hold values from -6 to 6
- grad_out: bfloat16 [8192, 13824], P(('depth', 'row'), 'col'), may hold values from -6 to 6
- weight: bfloat16 [5120, 13824], P('row', 'col'), may hold values from -0.078125 to 0.078125
- master: float32 [5120, 13824], P(('row', 'depth'), 'col'), may hold values from -0.078125 to 0.078125
- moment_one: float32 [5120, 13824], P(('row', 'depth'), 'col'), may hold values from -4 to 4
- moment_two: float32 [5120, 13824], P(('row', 'depth'), 'col'), may hold values from 0.05 to 2
Outputs:
- grad_in: bfloat16 [8192, 5120], P(('depth', 'col'), 'row')
- new_weight: bfloat16 [5120, 13824], P('row', 'col')
- new_master: float32 [5120, 13824], P(('row', 'depth'), 'col')
- new_moment_one: float32 [5120, 13824], P(('row', 'depth'), 'col')
- new_moment_two: float32 [5120, 13824], P(('row', 'depth'), 'col')
The draws below stay inside these ranges and needn't reach their ends.
All inputs are finite; a program needn't handle non-finite values.
Results may differ from the reference program's by a relative error of at most 0.0035.
Values may be sent and summed in bfloat16 or wider, within the bound.
A program may use at most 128 MiB of HBM per device.

```python
import math
import jax
import jax.numpy as jnp
from jax import lax

D = 5120
FF = 13824
STEP = 10
TOKENS = 8192


def levels(own_key, dims, split, smallest, high):
    def one(position, blocks):
        draws = jax.random.uniform(jax.random.fold_in(jax.random.fold_in(own_key, 6), position), (blocks,), jnp.float32, smallest / len(split), high / len(split))
        return jnp.repeat(jnp.exp(draws), dims[position] // blocks).reshape((-1,) + (1,) * (len(dims) - position - 1))

    gain = one(*split[0])
    for cut in split[1:]:
        gain = gain * one(*cut)
    return gain


def gaussian(rng, shape, width, bound, pieces=(), held_as=jnp.bfloat16):
    drawn = jax.random.normal(rng, shape, jnp.float32) * width
    if len(pieces) > 0:
        drawn = levels(rng, shape, pieces, -0.22, 0.18) * drawn
    return jnp.clip(drawn, min=-bound, max=bound).astype(held_as)


def setup_inputs(seed: int = 0) -> dict:
    seeds = jax.random.split(jax.random.key(seed), 7)
    return {
        "acts": gaussian(seeds[0], (TOKENS, D), 1.0, 6.0, ((0, 16), (1, 8))),
        "grad_out": gaussian(seeds[1], (TOKENS, FF), 1.0, 6.0, ((0, 32), (1, 4))),
        "weight": gaussian(seeds[2], (D, FF), D ** -0.5, 0.078125, ((0, 8), (1, 4))),
        "master": gaussian(seeds[3], (D, FF), D ** -0.5, 0.078125, ((0, 32), (1, 4)), jnp.float32),
        "moment_one": gaussian(seeds[4], (D, FF), 0.3, 4.0, ((0, 32), (1, 4)), jnp.float32),
        "moment_two": jnp.clip(jnp.exp(math.log(2.0) - 3.6888794 * jax.random.uniform(seeds[5], (D, FF), jnp.float32) ** levels(seeds[5], (D, FF), ((0, 32), (1, 4)), -0.2, 0.2)), 0.05, 2.0),
    }


def reference(acts, grad_out, weight, master, moment_one, moment_two):
    grad_in = lax.dot_general(grad_out, weight, (((1,), (1,)), ((), ())), preferred_element_type=jnp.float32).astype(jnp.bfloat16)
    grad = lax.dot_general(acts, grad_out, (((0,), (0,)), ((), ())), preferred_element_type=jnp.float32)
    grad = grad * jnp.float32(1.0 / math.sqrt(TOKENS))
    new_moment_one = 0.9 * moment_one + 0.1 * grad
    new_moment_two = 0.95 * moment_two + 0.05 * grad * grad
    first_fix = 1.0 - 0.9 ** STEP
    second_fix = 1.0 - 0.95 ** STEP
    update = new_moment_one / first_fix / (jnp.sqrt(new_moment_two / second_fix) + 1e-08)
    new_master = master - 0.01 * (update + 0.1 * master)
    new_weight = new_master.astype(jnp.bfloat16)
    return (grad_in, new_weight, new_master, new_moment_one, new_moment_two)
```

```python
import math

import jax
import jax.numpy as jnp
from jax import lax
from jax.experimental import pallas as pl
from jax.experimental.pallas import tpu as pltpu
from jax.sharding import PartitionSpec as P

STEP = 10
WC = 384
MESH = pl.DeviceIdType.MESH
F32, BF16 = jnp.float32, jnp.bfloat16


def place():
    r, c, d = lax.axis_index("row"), lax.axis_index("col"), lax.axis_index("depth")
    return r // 2, lax.rem(r, 2), c // 2, lax.rem(c, 2), d


def adamw(grad, master, one, two):
    new_one = 0.9 * one + 0.1 * grad
    new_two = 0.95 * two + 0.05 * grad * grad
    first_fix = 1.0 - 0.9**STEP
    second_fix = 1.0 - 0.95**STEP
    update = new_one / first_fix / (jnp.sqrt(new_two / second_fix) + 1e-08)
    return master - 0.01 * (update + 0.1 * master), new_one, new_two


def kernel(
    nc, scale,
    acts, grad_out, weight, master, moment_one, moment_two,
    grad_in, new_weight, new_master, new_one, new_two,
    G, W, ACT, AT, GI, D2D, SB, RB, GO, GS, RS, OPT, NW,
    g_sem, w_sem, a_sem, o_sem, out_sem, nw_sem, gi_sem,
    ts, tr, acs, acr, rss, rsr, ags, agr, ds, dr, zs, zr,
):
    x, h, zl, k, d = place()
    me = x * 2 + h
    col = zl * 2 + k
    xr, xl = lax.rem(x + 1, 4), lax.rem(x + 3, 4)
    left, right = xl * 2 + h, xr * 2 + h
    anti = lax.rem(x + 2, 4) * 2 + h
    zpart = x * 2 + (1 - h)
    dup, ddn, dan = lax.rem(d + 1, 4), lax.rem(d + 3, 4), lax.rem(d + 2, 4)

    d_right, d_left = (right, col, d), (left, col, d)
    d_zp = (zpart, col, d)
    d_core = (me, zl * 2 + (1 - k), d)
    d_zl = (me, (1 - zl) * 2 + k, d)
    d_up, d_dn, d_an = (me, col, dup), (me, col, ddn), (me, col, dan)

    def cols(c):
        return pl.ds(pl.multiple_of(c * WC, WC), WC)

    def load_g(c):
        return pltpu.make_async_copy(grad_out.at[:, cols(c)], G.at[c, me], g_sem.at[c])

    def load_w(c):
        return pltpu.make_async_copy(weight.at[:, cols(c)], W.at[c], w_sem.at[c])

    def load_o(c):
        return [
            pltpu.make_async_copy(ref.at[:, cols(c)], OPT.at[c, n], o_sem.at[c, n])
            for n, ref in enumerate((master, moment_one, moment_two))
        ]

    def store_o(c):
        return [
            pltpu.make_async_copy(OPT.at[c, n], ref.at[:, cols(c)], out_sem.at[c, n])
            for n, ref in enumerate((new_master, new_one, new_two))
        ]

    def store_w(c):
        return [
            pltpu.make_async_copy(
                NW.at[c, p], new_weight.at[pl.ds(p * 160, 160), cols(c)], nw_sem.at[c, p]
            )
            for p in range(4)
        ]

    load_a = pltpu.make_async_copy(acts, ACT.at[col], a_sem.at[0])

    load_g(0).start()
    load_a.start()
    load_g(1).start()

    barrier = pltpu.get_barrier_semaphore()
    for peer in (d_right, d_left, d_zp, d_core, d_zl, d_up, d_dn, d_an):
        pl.semaphore_signal(barrier, inc=1, device_id=peer, device_id_type=MESH)

    @pl.loop(2, nc)
    def _(c):
        load_g(c).start()

    @pl.loop(0, nc)
    def _(c):
        load_w(c).start()

    @pl.loop(0, nc)
    def _(c):
        for copy in load_o(c):
            copy.start()

    pl.semaphore_wait(barrier, 8)

    LO, HI, ALL = pl.ds(0, 128), pl.ds(128, 128), pl.ds(0, 256)

    def flow(n, c):
        slot, rows, peer = (
            (me, ALL, d_right), (me, ALL, d_left), (me, ALL, d_zp),
            (left, LO, d_right), (right, HI, d_left),
            (zpart, ALL, d_right), (zpart, ALL, d_left),
            (anti, LO, d_zp), (anti, HI, d_zp),
        )[n]
        ref = G.at[c, slot, rows]
        return pltpu.make_async_remote_copy(
            ref, ref, ts.at[c, n], tr.at[c, n], device_id=peer, device_id_type=MESH
        )

    def arrived(n, c):
        flow(n, c).wait_recv()

    def act_flow(n):
        slot, peer = ((col, d_zl), (col, d_core), ((1 - zl) * 2 + k, d_core))[n]
        ref = ACT.at[slot]
        return pltpu.make_async_remote_copy(
            ref, ref, acs.at[n], acr.at[n], device_id=peer, device_id_type=MESH
        )

    def rs_flow(n, c):
        piece, peer = ((dup, d_up), (dan, d_an), (ddn, d_dn))[n]
        return pltpu.make_async_remote_copy(
            GS.at[c, piece], RS.at[c, n], rss.at[c, n], rsr.at[c, n],
            device_id=peer, device_id_type=MESH,
        )

    def ag_flow(n, c):
        piece, rows, peer = (
            (d, pl.ds(0, 160), d_up), (d, pl.ds(0, 160), d_dn),
            (ddn, pl.ds(0, 80), d_up), (dup, pl.ds(80, 80), d_dn),
        )[n]
        ref = NW.at[c, piece, rows]
        return pltpu.make_async_remote_copy(
            ref, ref, ags.at[c, n], agr.at[c, n], device_id=peer, device_id_type=MESH
        )

    def core_flow(n):
        return pltpu.make_async_remote_copy(
            GI.at[n * 2 + (1 - k)], D2D.at[n], ds.at[n], dr.at[n],
            device_id=d_core, device_id_type=MESH,
        )

    zl_flow = pltpu.make_async_remote_copy(
        SB, RB, zs.at[0], zr.at[0], device_id=d_zl, device_id_type=MESH
    )

    def own_sends(c):
        load_g(c).wait()
        flow(2, c).start()
        flow(0, c).start()
        flow(1, c).start()

    own_sends(0)
    load_a.wait()
    act_flow(0).start()
    act_flow(1).start()
    own_sends(1)

    GI[...] = jnp.zeros_like(GI)

    def turn_acts(slot):
        AT[:, pl.ds(pl.multiple_of(slot * 512, 512), 512)] = ACT[slot].T

    def input_sums(c):
        @pl.loop(0, 4)
        def _(o):
            g = G[c, pl.ds(o * 2, 2)].reshape(512, WC)
            GI[o] += lax.dot_general(
                g, W[c], (((1,), (1,)), ((), ())), preferred_element_type=F32
            )

    def weight_grad(c):
        g = G[c].reshape(2048, WC)

        @pl.loop(0, 4)
        def _(p):
            rows = AT[pl.ds(pl.multiple_of(p * 160, 160), 160), :]
            GS[c, p] = jnp.dot(rows, g, preferred_element_type=F32).astype(BF16)

    @pl.loop(0, nc + 5)
    def _(i):
        @pl.when(i + 2 < nc)
        def _():
            own_sends(i + 2)

        @pl.when(i < nc)
        def _():
            arrived(2, i)
            flow(5, i).start()
            flow(6, i).start()
            arrived(0, i)
            flow(3, i).start()
            arrived(1, i)
            flow(4, i).start()

        @pl.when((i >= 1) & (i < nc + 1))
        def _():
            arrived(3, i - 1)
            flow(7, i - 1).start()
            arrived(4, i - 1)
            flow(8, i - 1).start()

        @pl.when(i == 1)
        def _():
            turn_acts(col)
            act_flow(1).wait_recv()
            turn_acts(zl * 2 + (1 - k))
            act_flow(0).wait_recv()
            act_flow(2).start()
            turn_acts((1 - zl) * 2 + k)

        @pl.when(i == 2)
        def _():
            act_flow(2).wait_recv()
            turn_acts((1 - zl) * 2 + (1 - k))

        @pl.when((i >= 2) & (i < nc + 2))
        def _():
            c = i - 2
            for n in (5, 6, 7, 8):
                arrived(n, c)
            load_w(c).wait()

            input_sums(c)

            @pl.when(c == nc - 1)
            def _():
                core_flow(0).start()
                core_flow(1).start()

            weight_grad(c)
            for n in range(3):
                rs_flow(n, c).start()

            @pl.when(c == nc - 1)
            def _():
                core_flow(0).wait_recv()
                core_flow(1).wait_recv()
                SB[...] = (GI[(1 - zl) * 2 + k] + D2D[1 - zl]).astype(BF16)
                zl_flow.start()

        @pl.when((i >= 3) & (i < nc + 3))
        def _():
            c = i - 3
            for n in range(3):
                rs_flow(n, c).wait_recv()
            for copy in load_o(c):
                copy.wait()
            grad = GS[c, d].astype(F32)
            for n in range(3):
                grad = grad + RS[c, n].astype(F32)
            a, b, e = adamw(grad * scale, OPT[c, 0], OPT[c, 1], OPT[c, 2])
            NW[c, d] = a.astype(BF16)
            OPT[c, 0] = a
            OPT[c, 1] = b
            OPT[c, 2] = e
            ag_flow(0, c).start()
            ag_flow(1, c).start()
            for copy in store_o(c):
                copy.start()

        @pl.when((i >= 4) & (i < nc + 4))
        def _():
            c = i - 4
            ag_flow(0, c).wait_recv()
            ag_flow(2, c).start()
            ag_flow(1, c).wait_recv()
            ag_flow(3, c).start()

        @pl.when(i >= 5)
        def _():
            c = i - 5
            ag_flow(2, c).wait_recv()
            ag_flow(3, c).wait_recv()
            for copy in store_w(c):
                copy.start()

    zl_flow.wait_recv()
    GO[...] = (GI[col] + D2D[zl] + RB[...].astype(F32)).astype(BF16)
    out = pltpu.make_async_copy(GO, grad_in, gi_sem.at[0])
    out.start()

    @pl.loop(0, nc)
    def _(c):
        for n in range(9):
            flow(n, c).wait_send()
        for n in range(3):
            rs_flow(n, c).wait_send()
        for n in range(4):
            ag_flow(n, c).wait_send()
        for copy in store_o(c) + store_w(c):
            copy.wait()

    for n in range(3):
        act_flow(n).wait_send()
    core_flow(0).wait_send()
    core_flow(1).wait_send()
    zl_flow.wait_send()
    out.wait()


def per_device(acts, grad_out, weight, master, moment_one, moment_two):
    tokens_total = acts.shape[0] * lax.axis_size("col") * lax.axis_size("depth")
    width = grad_out.shape[1]
    nc = width // WC
    scale = float(1.0 / math.sqrt(tokens_total))
    dma = pltpu.SemaphoreType.DMA
    anywhere = pl.BlockSpec(memory_space=pl.ANY)

    def body(*refs):
        kernel(nc, scale, *refs)

    return pl.pallas_call(
        body,
        out_shape=(
            jax.ShapeDtypeStruct(acts.shape, BF16),
            jax.ShapeDtypeStruct(weight.shape, BF16),
            jax.ShapeDtypeStruct(master.shape, F32),
            jax.ShapeDtypeStruct(master.shape, F32),
            jax.ShapeDtypeStruct(master.shape, F32),
        ),
        in_specs=[anywhere] * 6,
        out_specs=(anywhere,) * 5,
        scratch_shapes=[
            pltpu.VMEM((nc, 8, 256, WC), BF16),
            pltpu.VMEM((nc, 640, WC), BF16),
            pltpu.VMEM((4, 512, 640), BF16),
            pltpu.VMEM((640, 2048), BF16),
            pltpu.VMEM((4, 512, 640), F32),
            pltpu.VMEM((2, 512, 640), F32),
            pltpu.VMEM((512, 640), BF16),
            pltpu.VMEM((512, 640), BF16),
            pltpu.VMEM((512, 640), BF16),
            pltpu.VMEM((nc, 4, 160, WC), BF16),
            pltpu.VMEM((nc, 3, 160, WC), BF16),
            pltpu.VMEM((nc, 3, 160, WC), F32),
            pltpu.VMEM((nc, 4, 160, WC), BF16),
            dma((nc,)), dma((nc,)), dma((1,)), dma((nc, 3)), dma((nc, 3)), dma((nc, 4)), dma((1,)),
            dma((nc, 9)), dma((nc, 9)),
            dma((3,)), dma((3,)),
            dma((nc, 3)), dma((nc, 3)),
            dma((nc, 4)), dma((nc, 4)),
            dma((2,)), dma((2,)),
            dma((1,)), dma((1,)),
        ],
        compiler_params=pltpu.CompilerParams(
            collective_id=0, has_side_effects=True, vmem_limit_bytes=67_000_000
        ),
        name="step",
    )(acts, grad_out, weight, master, moment_one, moment_two)


def solution(mesh):
    placed = (
        P(("depth", "col"), "row"),
        P(("depth", "row"), "col"),
        P("row", "col"),
        P(("row", "depth"), "col"),
        P(("row", "depth"), "col"),
        P(("row", "depth"), "col"),
    )
    return jax.shard_map(
        per_device,
        mesh=mesh,
        in_specs=placed,
        out_specs=(
            P(("depth", "col"), "row"),
            P("row", "col"),
            P(("row", "depth"), "col"),
            P(("row", "depth"), "col"),
            P(("row", "depth"), "col"),
        ),
        check_vma=False,
    )
```

```python
import math

import jax
import jax.numpy as jnp
from jax import lax
from jax.experimental import pallas as pl
from jax.experimental.pallas import tpu as pltpu
from jax.sharding import PartitionSpec as P

STEP = 10
BY_X = 2
STRIP = 128
GROUP = 3
WIDE = STRIP * GROUP

MESH = pl.DeviceIdType.MESH
F32, BF16 = jnp.float32, jnp.bfloat16


def place():
    r, c, d = lax.axis_index("row"), lax.axis_index("col"), lax.axis_index("depth")
    return r // 2, lax.rem(r, 2), c // 2, lax.rem(c, 2), d


def adamw(grad, master, one, two):
    new_one = 0.9 * one + 0.1 * grad
    new_two = 0.95 * two + 0.05 * grad * grad
    first_fix = 1.0 - 0.9**STEP
    second_fix = 1.0 - 0.95**STEP
    update = new_one / first_fix / (jnp.sqrt(new_two / second_fix) + 1e-08)
    return master - 0.01 * (update + 0.1 * master), new_one, new_two


def kernel(
    nc, scale,
    acts, grad_out, weight, master, moment_one, moment_two,
    grad_in, new_weight, new_master, new_one, new_two,
    G, W, ACT, AT, GI, D2D, SB, RB, GS, RS,
    g_sem, w_sem, a_sem, o_sem,
    ts, tr, acs, acr, rss, rsr, ags, agr, ds, dr, zs, zr,
):
    x, h, zl, k, d = place()
    me = x * 2 + h
    col = zl * 2 + k
    xr, xl = lax.rem(x + 1, 4), lax.rem(x + 3, 4)
    left, right = xl * 2 + h, xr * 2 + h
    anti = lax.rem(x + 2, 4) * 2 + h
    zpart = x * 2 + (1 - h)
    left_zp, right_zp = xl * 2 + (1 - h), xr * 2 + (1 - h)
    dup, ddn, dan = lax.rem(d + 1, 4), lax.rem(d + 3, 4), lax.rem(d + 2, 4)

    d_right, d_left = (right, col, d), (left, col, d)
    d_zp = (zpart, col, d)
    d_core = (me, zl * 2 + (1 - k), d)
    d_zl = (me, (1 - zl) * 2 + k, d)
    d_up, d_dn = (me, col, dup), (me, col, ddn)

    last = nc - 1

    def strips(q):
        return pl.ds(q * GROUP, GROUP)

    def cols(q):
        return pl.ds(pl.multiple_of(q * WIDE, STRIP), WIDE)

    def load_g(q):
        return [
            pltpu.make_async_copy(
                grad_out.at[:, :, :, pl.ds(pl.multiple_of((q * GROUP + n) * STRIP, STRIP), STRIP)],
                G.at[q * GROUP + n, me],
                g_sem.at[q, n],
            )
            for n in range(GROUP)
        ]

    def load_o(n):
        ref, to = ((master, new_master), (moment_one, new_one), (moment_two, new_two))[n]
        return pltpu.make_async_copy(ref, to, o_sem.at[n])

    load_w = pltpu.make_async_copy(weight, W, w_sem.at[0])
    load_a = pltpu.make_async_copy(acts, ACT.at[col], a_sem.at[0])

    def start_g(q):
        for copy in load_g(q):
            copy.start()

    def loaded_g(q):
        for copy in load_g(q):
            copy.wait()

    start_g(0)
    start_g(1)
    load_a.start()

    barrier = pltpu.get_barrier_semaphore()
    for peer in (d_right, d_left, d_zp, d_core, d_zl, d_up, d_dn):
        pl.semaphore_signal(barrier, inc=1, device_id=peer, device_id_type=MESH)

    @pl.loop(2, nc)
    def _(q):
        start_g(q)

    load_w.start()
    for n in range(3):
        load_o(n).start()

    pl.semaphore_wait(barrier, 7)

    def flow(n, q, piece=None):
        slot, half, peer = (
            (me, None, d_right), (me, None, d_left), (me, None, d_zp),
            (left, 0, d_right), (right, 1, d_left),
            (zpart, None, d_right), (zpart, None, d_left),
            (anti, 0, d_zp), (anti, 1, d_zp),
            (left_zp, 0, d_right), (right_zp, 1, d_left),
        )[n]
        n = n - 2 if n > 8 else n
        ref = G.at[
            strips(q), slot,
            pl.ds(0, 2) if half is None else half,
            pl.ds(0, 2) if piece is None else piece,
        ]
        sem = q if piece is None else last + piece
        return pltpu.make_async_remote_copy(
            ref, ref, ts.at[sem, n], tr.at[sem, n], device_id=peer, device_id_type=MESH
        )

    def arrived(n, q, piece=None):
        flow(n, q, piece).wait_recv()

    def act_flow(n):
        slot, peer = ((col, d_zl), (col, d_core), ((1 - zl) * 2 + k, d_core))[n]
        ref = ACT.at[slot]
        return pltpu.make_async_remote_copy(
            ref, ref, acs.at[n], acr.at[n], device_id=peer, device_id_type=MESH
        )

    TOP, LOW = pl.ds(0, 80), pl.ds(80, 80)

    def rs_flow(n, q):
        piece, rows, slot, peer = (
            (dan, TOP, 2, d_up), (dan, LOW, 2, d_dn),
            (dup, LOW, 0, d_up), (ddn, TOP, 1, d_dn),
            (dup, TOP, 0, d_up), (ddn, LOW, 1, d_dn),
        )[n]
        at = strips(q)
        return pltpu.make_async_remote_copy(
            GS.at[at, piece, rows], RS.at[at, slot, rows], rss.at[q, n], rsr.at[q, n],
            device_id=peer, device_id_type=MESH,
        )

    def ag_flow(n, q):
        piece, first, count, peer = (
            (d, 0, 160, d_up), (d, 0, 160, d_dn), (ddn, 0, 80, d_up), (dup, 80, 80, d_dn),
        )[n]
        rows = pl.ds(pl.multiple_of(piece * 160 + first, 16), count)
        ref = new_weight.at[rows, cols(q)]
        return pltpu.make_async_remote_copy(
            ref, ref, ags.at[q, n], agr.at[q, n], device_id=peer, device_id_type=MESH
        )

    far, near = 1 - zl, zl

    def core_flow(n, piece):
        half = (far, near)[n]
        return pltpu.make_async_remote_copy(
            GI.at[half * 2 + (1 - k), :, piece], D2D.at[half, :, piece],
            ds.at[n, piece], dr.at[n, piece], device_id=d_core, device_id_type=MESH,
        )

    def zl_flow(n, piece):
        at = pl.ds(2 * n, 2)
        return pltpu.make_async_remote_copy(
            SB.at[at, piece], RB.at[at, piece], zs.at[n, piece], zr.at[n, piece],
            device_id=d_zl, device_id_type=MESH,
        )

    def forward_x(q, piece=None):
        flow(3, q, piece).start()
        flow(4, q, piece).start()

    def forward_z(q, piece=None):
        flow(5, q, piece).start()
        flow(6, q, piece).start()

    def onward_x(q, piece=None):
        arrived(5, q, piece)
        flow(9, q, piece).start()
        arrived(6, q, piece)
        flow(10, q, piece).start()

    def onward_z(q):
        arrived(3, q)
        flow(7, q).start()
        arrived(4, q)
        flow(8, q).start()

    def turn_acts(slot):
        AT[:, pl.ds(pl.multiple_of(slot * 512, 512), 512)] = ACT[slot].T

    def input_sums(q, first, count, piece=None):
        rows = 512 if piece is None else 256

        @pl.loop(first, first + count)
        def _(j):
            o = jnp.where(j < 2, far, near) * 2 + jnp.where(lax.rem(j, 2) == 0, 1 - k, k)
            slots = pl.ds(o * 2, 2)
            if piece is None:
                parts = [G[q * GROUP + n, slots] for n in range(GROUP)]
            else:
                parts = [G[q * GROUP + n, slots, :, piece] for n in range(GROUP)]
            g = jnp.concatenate([p.reshape(rows, STRIP) for p in parts], axis=1)
            out = lax.dot_general(
                g, W[:, cols(q)], (((1,), (1,)), ((), ())), preferred_element_type=F32
            )
            if piece is None:
                GI[o] += out.reshape(4, 2, 64, 640)
            else:
                GI[o, :, piece] += out.reshape(4, 64, 640)

    def weight_grad(q):
        g = jnp.concatenate([G[q * GROUP + n].reshape(2048, STRIP) for n in range(GROUP)], axis=1)

        @pl.loop(0, 4)
        def _(p):
            rows = AT[pl.ds(pl.multiple_of(p * 160, 160), 160), :]
            out = jnp.dot(rows, g, preferred_element_type=F32).astype(BF16)
            for n in range(GROUP):
                GS[q * GROUP + n, p] = out[:, n * STRIP:(n + 1) * STRIP]

    def send_pieces(q):
        for n in range(4):
            rs_flow(n, q).start()

    def join_pieces(q):
        rs_flow(0, q).wait_recv()
        rs_flow(1, q).wait_recv()

        @pl.loop(q * GROUP, (q + 1) * GROUP)
        def _(s):
            GS[s, dup, TOP] = (GS[s, dup, TOP].astype(F32) + RS[s, 2, TOP].astype(F32)).astype(BF16)
            GS[s, ddn, LOW] = (GS[s, ddn, LOW].astype(F32) + RS[s, 2, LOW].astype(F32)).astype(BF16)

        rs_flow(4, q).start()
        rs_flow(5, q).start()

    def update(q):
        for n in range(2, 6):
            rs_flow(n, q).wait_recv()
        @pl.loop(q * GROUP, (q + 1) * GROUP)
        def _(s):
            grad = GS[s, d].astype(F32) + RS[s, 0].astype(F32) + RS[s, 1].astype(F32)
            at = pl.ds(pl.multiple_of(s * STRIP, STRIP), STRIP)
            a, b, e = adamw(grad * scale, new_master[:, at], new_one[:, at], new_two[:, at])
            new_weight[pl.ds(pl.multiple_of(d * 160, 160), 160), at] = a.astype(BF16)
            new_master[:, at] = a
            new_one[:, at] = b
            new_two[:, at] = e
        ag_flow(0, q).start()
        ag_flow(1, q).start()

    def forward_w(q):
        ag_flow(0, q).wait_recv()
        ag_flow(2, q).start()
        ag_flow(1, q).wait_recv()
        ag_flow(3, q).start()

    def own_x(q):
        flow(0, q).start()
        flow(1, q).start()

    for q in range(2):
        loaded_g(q)
        flow(2, q).start()
        own_x(q)
    load_a.wait()
    act_flow(0).start()
    act_flow(1).start()
    for q in (2, 3):
        loaded_g(q)
        flow(2, q).start()

    GI[...] = jnp.zeros_like(GI)
    turn_acts(col)
    def x_arrived(q):
        arrived(0, q)
        arrived(1, q)

    def z_arrived(q):
        arrived(2, q)

    def by_x(q):
        return q < BY_X

    x_arrived(0)
    forward_x(0)
    z_arrived(0)
    forward_z(0)
    act_flow(1).wait_recv()
    turn_acts(zl * 2 + (1 - k))
    x_arrived(1)
    forward_x(1)
    z_arrived(1)
    forward_z(1)
    if BY_X > 0:
        onward_x(0)
    own_x(2)
    load_w.wait()
    for n in range(3):
        load_o(n).wait()

    @pl.loop(2, nc)
    def _(i):
        q = i - 2

        @pl.when(i == 2)
        def _():
            act_flow(0).wait_recv()
            act_flow(2).start()
            turn_acts((1 - zl) * 2 + k)
            if BY_X > 1:
                onward_x(1)

        @pl.when((i > 2) & (i < last))
        def _():
            z_arrived(i)
            forward_z(i)

        @pl.when(i == last)
        def _():
            z_arrived(last)
            forward_z(last, 0)

        @pl.when(i - 1 >= max(BY_X, 1))
        def _():
            onward_z(i - 1)

        @pl.when(i >= 3)
        def _():
            join_pieces(i - 3)

        @pl.when(i == 2)
        def _():
            act_flow(2).wait_recv()
            turn_acts((1 - zl) * 2 + (1 - k))
        @pl.when(by_x(q))
        def _():
            arrived(3, q)
            arrived(4, q)

        @pl.when(jnp.logical_not(by_x(q)))
        def _():
            arrived(5, q)
            arrived(6, q)

        arrived(7, q)
        arrived(8, q)
        input_sums(q, 0, 4)

        @pl.when(i == 2)
        def _():
            z_arrived(2)
            forward_z(2)

        x_arrived(i)

        @pl.when(i < last)
        def _():
            forward_x(i)
            own_x(i + 1)

        @pl.when(i == last)
        def _():
            forward_x(last, 0)
            forward_z(last, 1)
            forward_x(last, 1)

        @pl.when(i + 2 < nc)
        def _():
            loaded_g(i + 2)
            flow(2, i + 2).start()

        @pl.when(i >= 4)
        def _():
            forward_w(i - 4)
        weight_grad(q)
        send_pieces(q)

        @pl.when(i >= 3)
        def _():
            update(i - 3)

    def far_sums(piece):
        core_flow(0, piece).wait_recv()
        for n in range(2):
            at = pl.ds(2 * n, 2)
            SB[at, piece] = (GI[far * 2 + k, at, piece] + D2D[far, at, piece]).astype(BF16)

    onward_x(last, 0)
    for n in (5, 6, 7, 8):
        arrived(n, last - 1)
    input_sums(last - 1, 0, 4)
    onward_x(last, 1)
    weight_grad(last - 1)
    send_pieces(last - 1)
    join_pieces(last - 2)

    for piece in range(2):
        for n in (3, 4, 7, 8):
            arrived(n, last, piece)
        input_sums(last, 0, 2, piece)
        if piece == 0:
            core_flow(0, 0).start()
        input_sums(last, 2, 2, piece)
        if piece == 0:
            core_flow(1, 0).start()
            forward_w(last - 3)
    core_flow(0, 1).start()
    far_sums(0)
    core_flow(1, 1).start()
    zl_flow(0, 0).start()
    zl_flow(1, 0).start()
    weight_grad(last)
    send_pieces(last)
    far_sums(1)
    join_pieces(last - 1)
    zl_flow(0, 1).start()
    zl_flow(1, 1).start()
    update(last - 2)
    join_pieces(last)
    update(last - 1)
    forward_w(last - 2)
    update(last)
    forward_w(last - 1)
    forward_w(last)
    @pl.loop(0, nc)
    def _(q):
        ag_flow(2, q).wait_recv()
        ag_flow(3, q).wait_recv()
    for piece in range(2):
        core_flow(1, piece).wait_recv()
        for n in range(2):
            zl_flow(n, piece).wait_recv()
            at = pl.ds(2 * n, 2)
            total = GI[col, at, piece] + D2D[near, at, piece] + RB[at, piece].astype(F32)
            grad_in[at, piece] = total.astype(BF16)

    @pl.loop(0, nc)
    def _(q):
        for m in range(3):
            flow(m, q).wait_send()
        for m in range(6):
            rs_flow(m, q).wait_send()
        for m in range(4):
            ag_flow(m, q).wait_send()

    @pl.loop(0, last)
    def _(q):
        for m in range(3, 9):
            flow(m, q).wait_send()

    for piece in range(2):
        for m in range(3, 9):
            flow(m, last, piece).wait_send()
        for n in range(2):
            core_flow(n, piece).wait_send()
            zl_flow(n, piece).wait_send()

    for n in range(3):
        act_flow(n).wait_send()


def write_out(*refs):
    held, outs, sems = refs[:5], refs[5:10], refs[10]
    copies = [pltpu.make_async_copy(a, b, sems.at[n]) for n, (a, b) in enumerate(zip(held, outs))]
    for copy in copies:
        copy.start()
    for copy in copies:
        copy.wait()


def per_device(acts, grad_out, weight, master, moment_one, moment_two):
    tokens_total = acts.shape[0] * lax.axis_size("col") * lax.axis_size("depth")
    width = grad_out.shape[1]
    strips = width // STRIP
    nc = strips // GROUP
    scale = float(1.0 / math.sqrt(tokens_total))
    dma = pltpu.SemaphoreType.DMA
    anywhere = pl.BlockSpec(memory_space=pl.ANY)
    on_chip = pl.BlockSpec(memory_space=pltpu.VMEM)

    def body(*refs):
        kernel(nc, scale, *refs)

    results = [((4, 2, 64, 640), BF16), (weight.shape, BF16)] + [(master.shape, F32)] * 3
    held = pl.pallas_call(
        body,
        out_shape=tuple(pltpu.VMEM(*r) for r in results),
        in_specs=[anywhere] * 6,
        out_specs=(on_chip,) * 5,
        scratch_shapes=[
            pltpu.VMEM((strips, 8, 2, 2, 64, STRIP), BF16),
            pltpu.VMEM((640, width), BF16),
            pltpu.VMEM((4, 512, 640), BF16),
            pltpu.VMEM((640, 2048), BF16),
            pltpu.VMEM((4, 4, 2, 64, 640), F32),
            pltpu.VMEM((2, 4, 2, 64, 640), F32),
            pltpu.VMEM((4, 2, 64, 640), BF16),
            pltpu.VMEM((4, 2, 64, 640), BF16),
            pltpu.VMEM((strips, 4, 160, STRIP), BF16),
            pltpu.VMEM((strips, 3, 160, STRIP), BF16),
            dma((nc, GROUP)), dma((1,)), dma((1,)), dma((3,)),
            dma((nc + 1, 9)), dma((nc + 1, 9)),
            dma((3,)), dma((3,)),
            dma((nc, 6)), dma((nc, 6)),
            dma((nc, 4)), dma((nc, 4)),
            dma((2, 2)), dma((2, 2)),
            dma((2, 2)), dma((2, 2)),
        ],
        compiler_params=pltpu.CompilerParams(
            collective_id=0, has_side_effects=True, vmem_limit_bytes=46 * 2**20
        ),
        name="step",
    )(acts, grad_out.reshape(2, 2, 64, width), weight, master, moment_one, moment_two)
    outs = pl.pallas_call(
        write_out,
        out_shape=tuple(jax.ShapeDtypeStruct(*r) for r in results),
        in_specs=[on_chip] * 5,
        out_specs=(anywhere,) * 5,
        scratch_shapes=[dma((5,))],
        compiler_params=pltpu.CompilerParams(vmem_limit_bytes=2**20),
        name="write_out",
    )(*[pltpu.with_memory_space_constraint(a, pltpu.VMEM) for a in held])
    return (outs[0].reshape(acts.shape), *outs[1:])


def solution(mesh):
    placed = (
        P(("depth", "col"), "row"),
        P(("depth", "row"), "col"),
        P("row", "col"),
        P(("row", "depth"), "col"),
        P(("row", "depth"), "col"),
        P(("row", "depth"), "col"),
    )
    return jax.shard_map(
        per_device,
        mesh=mesh,
        in_specs=placed,
        out_specs=(
            P(("depth", "col"), "row"),
            P("row", "col"),
            P(("row", "depth"), "col"),
            P(("row", "depth"), "col"),
            P(("row", "depth"), "col"),
        ),
        check_vma=False,
    )
```

```python
import math

import jax
import jax.numpy as jnp
from jax import lax
from jax.experimental import pallas as pl
from jax.experimental.pallas import tpu as pltpu
from jax.sharding import PartitionSpec as P

STEP = 10
PARTS = 2
BY_X = 1
STRIP = 128
GROUP = 2
LAST = 3
FIRST = 3
AHEAD = 2
WIDE = STRIP * GROUP
MESH = pl.DeviceIdType.MESH
F32, BF16 = jnp.float32, jnp.bfloat16


def place():
    r, c, d = lax.axis_index("row"), lax.axis_index("col"), lax.axis_index("depth")
    return r // 2, lax.rem(r, 2), c // 2, lax.rem(c, 2), d


def adamw(grad, master, one, two):
    new_one = 0.9 * one + 0.1 * grad
    new_two = 0.95 * two + 0.05 * grad * grad
    first_fix = 1.0 - 0.9**STEP
    second_fix = 1.0 - 0.95**STEP
    update = new_one / first_fix / (jnp.sqrt(new_two / second_fix) + 1e-08)
    return master - 0.01 * (update + 0.1 * master), new_one, new_two


def kernel(
    nc, scale,
    acts, grad_out, weight, master, moment_one, moment_two,
    grad_in, new_weight, new_master, new_one, new_two,
    G, W, ACT, AT, GI, D2D, SB, RB, GS, RS,
    g_sem, w_sem, a_sem, o_sem,
    ts, tr, acs, acr, rss, rsr, ags, agr, ds, dr, zs, zr,
):
    x, h, zl, k, d = place()
    me = x * 2 + h
    col = zl * 2 + k
    xr, xl = lax.rem(x + 1, 4), lax.rem(x + 3, 4)
    left, right = xl * 2 + h, xr * 2 + h
    anti = lax.rem(x + 2, 4) * 2 + h
    zpart = x * 2 + (1 - h)
    left_zp, right_zp = xl * 2 + (1 - h), xr * 2 + (1 - h)
    dup, ddn, dan = lax.rem(d + 1, 4), lax.rem(d + 3, 4), lax.rem(d + 2, 4)

    d_right, d_left = (right, col, d), (left, col, d)
    d_zp = (zpart, col, d)
    d_core = (me, zl * 2 + (1 - k), d)
    d_zl = (me, (1 - zl) * 2 + k, d)
    d_up, d_dn = (me, col, dup), (me, col, ddn)

    last = nc - 1

    def size(q):
        return LAST if isinstance(q, int) and q == last else GROUP

    def strips(q):
        return pl.ds(q * GROUP, size(q))

    def cols(q):
        return pl.ds(pl.multiple_of(q * WIDE, STRIP), size(q) * STRIP)

    def load_g(q):
        return [
            pltpu.make_async_copy(
                grad_out.at[:, :, :, pl.ds(pl.multiple_of((q * GROUP + n) * STRIP, STRIP), STRIP)],
                G.at[q * GROUP + n, me],
                g_sem.at[q, n],
            )
            for n in range(size(q))
        ]

    def load_o(n):
        ref, to = ((master, new_master), (moment_one, new_one), (moment_two, new_two))[n]
        return pltpu.make_async_copy(ref, to, o_sem.at[n])

    load_w = pltpu.make_async_copy(weight, W, w_sem.at[0])
    load_a = pltpu.make_async_copy(acts, ACT.at[col], a_sem.at[0])

    def start_g(q):
        for copy in load_g(q):
            copy.start()

    def loaded_g(q):
        for copy in load_g(q):
            copy.wait()

    start_g(0)
    start_g(1)
    load_a.start()

    barrier = pltpu.get_barrier_semaphore()
    for peer in (d_right, d_left, d_zp, d_core, d_zl, d_up, d_dn):
        pl.semaphore_signal(barrier, inc=1, device_id=peer, device_id_type=MESH)

    @pl.loop(2, last)
    def _(q):
        start_g(q)

    start_g(last)
    load_w.start()
    for n in range(3):
        load_o(n).start()

    pl.semaphore_wait(barrier, 7)

    def flow(n, q, piece=None):
        slot, half, peer = (
            (me, None, d_right), (me, None, d_left), (me, None, d_zp),
            (left, 0, d_right), (right, 1, d_left),
            (zpart, None, d_right), (zpart, None, d_left),
            (anti, 0, d_zp), (anti, 1, d_zp),
            (left_zp, 0, d_right), (right_zp, 1, d_left),
        )[n]
        n = n - 2 if n > 8 else n
        ref = G.at[
            strips(q), slot,
            pl.ds(0, 2) if half is None else half,
            pl.ds(0, 2) if piece is None else piece,
        ]
        sem = q if piece is None else last + piece
        return pltpu.make_async_remote_copy(
            ref, ref, ts.at[sem, n], tr.at[sem, n], device_id=peer, device_id_type=MESH
        )

    def arrived(n, q, piece=None):
        flow(n, q, piece).wait_recv()

    def act_flow(n):
        slot, peer = ((col, d_zl), (col, d_core), ((1 - zl) * 2 + k, d_core))[n]
        ref = ACT.at[slot]
        return pltpu.make_async_remote_copy(
            ref, ref, acs.at[n], acr.at[n], device_id=peer, device_id_type=MESH
        )

    TOP, LOW = pl.ds(0, 80), pl.ds(80, 80)

    def rs_flow(n, q):
        piece, rows, slot, peer = (
            (dan, TOP, 2, d_up), (dan, LOW, 2, d_dn),
            (dup, LOW, 0, d_up), (ddn, TOP, 1, d_dn),
            (dup, TOP, 0, d_up), (ddn, LOW, 1, d_dn),
        )[n]
        at = strips(q)
        return pltpu.make_async_remote_copy(
            GS.at[at, piece, rows], RS.at[at, slot, rows], rss.at[q, n], rsr.at[q, n],
            device_id=peer, device_id_type=MESH,
        )

    def ag_flow(n, q):
        piece, first, peer = (
            (d, 0, d_up), (d, 80, d_dn), (d, 80, d_up), (d, 0, d_dn),
            (ddn, 0, d_up), (dup, 80, d_dn),
        )[n]
        rows = pl.ds(pl.multiple_of(piece * 160 + first, 16), 80)
        ref = new_weight.at[rows, cols(q)]
        return pltpu.make_async_remote_copy(
            ref, ref, ags.at[q, n], agr.at[q, n], device_id=peer, device_id_type=MESH
        )

    far, near = 1 - zl, zl

    def core_flow(n, piece):
        half = (far, near)[n]
        return pltpu.make_async_remote_copy(
            GI.at[half * 2 + (1 - k), :, piece], D2D.at[half, :, piece],
            ds.at[n, piece], dr.at[n, piece], device_id=d_core, device_id_type=MESH,
        )

    def zl_flow(n, piece):
        at = pl.ds(2 * n, 2)
        return pltpu.make_async_remote_copy(
            SB.at[at, piece], RB.at[at, piece], zs.at[n, piece], zr.at[n, piece],
            device_id=d_zl, device_id_type=MESH,
        )

    def forward_x(q, piece=None):
        flow(3, q, piece).start()
        flow(4, q, piece).start()

    def forward_z(q, piece=None):
        flow(5, q, piece).start()
        flow(6, q, piece).start()

    def onward_x(q, piece=None):
        arrived(5, q, piece)
        flow(9, q, piece).start()
        arrived(6, q, piece)
        flow(10, q, piece).start()

    def onward_z(q):
        arrived(3, q)
        flow(7, q).start()
        arrived(4, q)
        flow(8, q).start()

    def turn_acts(slot):
        AT[:, pl.ds(pl.multiple_of(slot * 512, 512), 512)] = ACT[slot].T

    def side_by_side(parts):
        return parts[0] if len(parts) == 1 else jnp.concatenate(parts, axis=1)

    def input_sums(q, first, count, piece=None):
        rows = 512 if piece is None else 256

        @pl.loop(first, first + count)
        def _(j):
            o = jnp.where(j < 2, far, near) * 2 + jnp.where(lax.rem(j, 2) == 0, 1 - k, k)
            slots = pl.ds(o * 2, 2)
            if piece is None:
                parts = [G[q * GROUP + n, slots] for n in range(size(q))]
            else:
                parts = [G[q * GROUP + n, slots, :, piece] for n in range(size(q))]
            g = side_by_side([p.reshape(rows, STRIP) for p in parts])
            out = lax.dot_general(
                g, W[:, cols(q)], (((1,), (1,)), ((), ())), preferred_element_type=F32
            )
            if piece is None:
                GI[o] += out.reshape(4, 2, 64, 640)
            else:
                GI[o, :, piece] += out.reshape(4, 64, 640)

    def weight_grad(q):
        g = side_by_side([G[q * GROUP + n].reshape(2048, STRIP) for n in range(size(q))])

        @pl.loop(0, 4)
        def _(p):
            rows = AT[pl.ds(pl.multiple_of(p * 160, 160), 160), :]
            out = jnp.dot(rows, g, preferred_element_type=F32).astype(BF16)
            for n in range(size(q)):
                GS[q * GROUP + n, p] = out[:, n * STRIP:(n + 1) * STRIP]

    def send_pieces(q):
        for n in range(4):
            rs_flow(n, q).start()

    def join_pieces(q):
        rs_flow(0, q).wait_recv()
        rs_flow(1, q).wait_recv()

        @pl.loop(q * GROUP, q * GROUP + size(q))
        def _(s):
            GS[s, dup, TOP] = (GS[s, dup, TOP].astype(F32) + RS[s, 2, TOP].astype(F32)).astype(BF16)
            GS[s, ddn, LOW] = (GS[s, ddn, LOW].astype(F32) + RS[s, 2, LOW].astype(F32)).astype(BF16)

        rs_flow(4, q).start()
        rs_flow(5, q).start()

    def update(q):
        for n in range(2, 6):
            rs_flow(n, q).wait_recv()
        @pl.loop(q * GROUP, q * GROUP + size(q))
        def _(s):
            grad = GS[s, d].astype(F32) + RS[s, 0].astype(F32) + RS[s, 1].astype(F32)
            at = pl.ds(pl.multiple_of(s * STRIP, STRIP), STRIP)
            a, b, e = adamw(grad * scale, new_master[:, at], new_one[:, at], new_two[:, at])
            new_weight[pl.ds(pl.multiple_of(d * 160, 160), 160), at] = a.astype(BF16)
            new_master[:, at] = a
            new_one[:, at] = b
            new_two[:, at] = e
        for n in range(4):
            ag_flow(n, q).start()

    def forward_w(q):
        ag_flow(0, q).wait_recv()
        ag_flow(4, q).start()
        ag_flow(1, q).wait_recv()
        ag_flow(5, q).start()

    def own_x(q):
        flow(0, q).start()
        flow(1, q).start()

    for q in range(2):
        loaded_g(q)
        flow(2, q).start()
        own_x(q)
    if FIRST > 2:
        loaded_g(2)
        flow(2, 2).start()
    load_a.wait()
    act_flow(0).start()
    act_flow(1).start()
    for q in range(FIRST, FIRST + 2):
        loaded_g(q)
        flow(2, q).start()

    GI[...] = jnp.zeros_like(GI)
    turn_acts(col)
    def x_arrived(q):
        arrived(0, q)
        arrived(1, q)

    def z_arrived(q):
        arrived(2, q)

    def by_x(q):
        return q < BY_X

    def compute(q, between):
        if isinstance(q, int):
            skip = (3, 4) if q < BY_X else (5, 6)
            arrived(skip[0], q)
            arrived(skip[1], q)
        else:
            @pl.when(q < BY_X)
            def _():
                arrived(3, q)
                arrived(4, q)

            @pl.when(q >= BY_X)
            def _():
                arrived(5, q)
                arrived(6, q)

        arrived(7, q)
        arrived(8, q)
        input_sums(q, 0, 4)
        between()
        weight_grad(q)
        send_pieces(q)

    def onward(q):
        onward_x(q) if q < BY_X else onward_z(q)

    x_arrived(0)
    forward_x(0)
    z_arrived(0)
    forward_z(0)
    if AHEAD > 1:
        own_x(2)
    act_flow(1).wait_recv()
    turn_acts(zl * 2 + (1 - k))
    x_arrived(1)
    forward_x(1)
    z_arrived(1)
    forward_z(1)
    onward(0)
    own_x(2) if AHEAD < 2 else own_x(3)
    if FIRST > 2:
        z_arrived(2)
        forward_z(2)
        onward(1)
        loaded_g(FIRST + 2)
        flow(2, FIRST + 2).start()
        x_arrived(2)
        forward_x(2)
        own_x(2 + AHEAD)
    load_w.wait()
    for n in range(3):
        load_o(n).wait()
    act_flow(0).wait_recv()
    act_flow(2).start()
    turn_acts((1 - zl) * 2 + k)
    onward(FIRST - 1)
    act_flow(2).wait_recv()
    turn_acts((1 - zl) * 2 + (1 - k))
    def forward_first():
        z_arrived(FIRST)
        forward_z(FIRST)
        x_arrived(FIRST)
        forward_x(FIRST)
        own_x(FIRST + AHEAD)

    compute(0, forward_first)

    @pl.loop(FIRST, nc)
    def _(i):
        @pl.when(i > FIRST)
        def _():
            onward_z(i - 1)

        @pl.when(i > FIRST)
        def _():
            join_pieces(i - 3)

        @pl.when(i == FIRST + 1)
        def _():
            update(0)

        def between():
            @pl.when((i > FIRST) & (i < last))
            def _():
                x_arrived(i)
                forward_x(i)

            @pl.when((i > FIRST) & (i + AHEAD < last))
            def _():
                own_x(i + AHEAD)

            @pl.when(i + AHEAD == last)
            def _():
                own_x(last)

            @pl.when(i + 1 < last)
            def _():
                z_arrived(i + 1)
                forward_z(i + 1)

            @pl.when(i + 1 == last)
            def _():
                z_arrived(last)
                forward_z(last, 0)

            @pl.when(i == last)
            def _():
                x_arrived(last)
                forward_x(last, 0)
                forward_z(last, 1)
                forward_x(last, 1)

            @pl.when(i + 3 < last)
            def _():
                loaded_g(i + 3)
                flow(2, i + 3).start()

            @pl.when(i + 3 == last)
            def _():
                loaded_g(last)
                flow(2, last).start()

            @pl.when(i == FIRST)
            def _():
                join_pieces(0)

            @pl.when(i == FIRST + 2)
            def _():
                forward_w(0)

            @pl.when(i >= FIRST + 2)
            def _():
                forward_w(i - 4)

        compute(i - 2, between)

        @pl.when(i > FIRST)
        def _():
            update(i - 3)

    def far_sums(piece):
        core_flow(0, piece).wait_recv()
        for n in range(2):
            at = pl.ds(2 * n, 2)
            SB[at, piece] = (GI[far * 2 + k, at, piece] + D2D[far, at, piece]).astype(BF16)

    onward_x(last, 0)
    compute(last - 1, lambda: onward_x(last, 1))
    join_pieces(last - 2)

    def last_sums(piece):
        input_sums(last, 0, 2, piece)
        core_flow(0, piece).start()
        input_sums(last, 2, 2, piece)
        core_flow(1, piece).start()
    for n in (3, 4, 7, 8):
        arrived(n, last, 0)
    last_sums(0)
    forward_w(last - 3)
    for n in (3, 4, 7, 8):
        arrived(n, last, 1)
    weight_grad(last)
    far_sums(0)
    send_pieces(last)
    zl_flow(0, 0).start()
    zl_flow(1, 0).start()
    last_sums(1)
    join_pieces(last - 1)
    far_sums(1)
    update(last - 2)
    zl_flow(0, 1).start()
    zl_flow(1, 1).start()
    join_pieces(last)
    update(last - 1)
    forward_w(last - 2)
    update(last)
    forward_w(last - 1)
    forward_w(last)
    @pl.loop(0, last)
    def _(q):
        for n in range(2, 6):
            ag_flow(n, q).wait_recv()

    for n in range(2, 6):
        ag_flow(n, last).wait_recv()
    for piece in range(2):
        core_flow(1, piece).wait_recv()
        for n in range(2):
            zl_flow(n, piece).wait_recv()
            at = pl.ds(2 * n, 2)
            total = GI[col, at, piece] + D2D[near, at, piece] + RB[at, piece].astype(F32)
            grad_in[at, piece] = total.astype(BF16)

    def sent(q):
        for m in range(3):
            flow(m, q).wait_send()
        for m in range(6):
            rs_flow(m, q).wait_send()
            ag_flow(m, q).wait_send()

    @pl.loop(0, last)
    def _(q):
        sent(q)
        for m in range(3, 9):
            flow(m, q).wait_send()

    sent(last)
    for piece in range(2):
        for m in range(3, 9):
            flow(m, last, piece).wait_send()
        for n in range(2):
            core_flow(n, piece).wait_send()
            zl_flow(n, piece).wait_send()

    for n in range(3):
        act_flow(n).wait_send()


def write_out(*refs):
    held, outs, sems = refs[:5], refs[5:10], refs[10]
    pairs = [(held[0], outs[0])]
    for a, b in zip(held[1:], outs[1:]):
        part = a.shape[0] // PARTS
        rows = [pl.ds(n * part, part) for n in range(PARTS)]
        pairs += [(a.at[r], b.at[r]) for r in rows]
    copies = [pltpu.make_async_copy(a, b, sems.at[n]) for n, (a, b) in enumerate(pairs)]
    for copy in copies:
        copy.start()
    for copy in copies:
        copy.wait()


def per_device(acts, grad_out, weight, master, moment_one, moment_two):
    tokens_total = acts.shape[0] * lax.axis_size("col") * lax.axis_size("depth")
    width = grad_out.shape[1]
    strips = width // STRIP
    nc = (strips - LAST) // GROUP + 1
    scale = float(1.0 / math.sqrt(tokens_total))
    dma = pltpu.SemaphoreType.DMA
    anywhere = pl.BlockSpec(memory_space=pl.ANY)
    on_chip = pl.BlockSpec(memory_space=pltpu.VMEM)

    def body(*refs):
        kernel(nc, scale, *refs)

    results = [((4, 2, 64, 640), BF16), (weight.shape, BF16)] + [(master.shape, F32)] * 3
    held = pl.pallas_call(
        body,
        out_shape=tuple(pltpu.VMEM(*r) for r in results),
        in_specs=[anywhere] * 6,
        out_specs=(on_chip,) * 5,
        scratch_shapes=[
            pltpu.VMEM((strips, 8, 2, 2, 64, STRIP), BF16),
            pltpu.VMEM((640, width), BF16),
            pltpu.VMEM((4, 512, 640), BF16),
            pltpu.VMEM((640, 2048), BF16),
            pltpu.VMEM((4, 4, 2, 64, 640), F32),
            pltpu.VMEM((2, 4, 2, 64, 640), F32),
            pltpu.VMEM((4, 2, 64, 640), BF16),
            pltpu.VMEM((4, 2, 64, 640), BF16),
            pltpu.VMEM((strips, 4, 160, STRIP), BF16),
            pltpu.VMEM((strips, 3, 160, STRIP), BF16),
            dma((nc, max(GROUP, LAST))), dma((1,)), dma((1,)), dma((3,)),
            dma((nc + 1, 9)), dma((nc + 1, 9)),
            dma((3,)), dma((3,)),
            dma((nc, 6)), dma((nc, 6)),
            dma((nc, 6)), dma((nc, 6)),
            dma((2, 2)), dma((2, 2)),
            dma((2, 2)), dma((2, 2)),
        ],
        compiler_params=pltpu.CompilerParams(
            collective_id=0, has_side_effects=True, vmem_limit_bytes=46 * 2**20
        ),
        name="step",
    )(acts, grad_out.reshape(2, 2, 64, width), weight, master, moment_one, moment_two)
    outs = pl.pallas_call(
        write_out,
        out_shape=tuple(jax.ShapeDtypeStruct(*r) for r in results),
        in_specs=[on_chip] * 5,
        out_specs=(anywhere,) * 5,
        scratch_shapes=[dma((1 + 4 * PARTS,))],
        compiler_params=pltpu.CompilerParams(vmem_limit_bytes=2**20),
        name="write_out",
    )(*[pltpu.with_memory_space_constraint(a, pltpu.VMEM) for a in held])
    return (outs[0].reshape(acts.shape), *outs[1:])


def solution(mesh):
    placed = (
        P(("depth", "col"), "row"),
        P(("depth", "row"), "col"),
        P("row", "col"),
        P(("row", "depth"), "col"),
        P(("row", "depth"), "col"),
        P(("row", "depth"), "col"),
    )
    return jax.shard_map(
        per_device,
        mesh=mesh,
        in_specs=placed,
        out_specs=(
            P(("depth", "col"), "row"),
            P("row", "col"),
            P(("row", "depth"), "col"),
            P(("row", "depth"), "col"),
            P(("row", "depth"), "col"),
        ),
        check_vma=False,
    )
```
